32 devices in a mesh: nodes: 16 (over z, y, x), feat: 2 (over core).
Axes of the slice: x: 2, y: 2, z: 4, core: 2. Of those that a mesh axis runs over, the one named last changes fastest.
Arguments:
- features: bfloat16 [8192, 128], P('nodes'), may hold values from -6 to 6
- row_counts: int32 [16], P('nodes'), may hold values from 128 to 512, as said below
- send_rows: int32 [16, 16, 64], P('nodes'), may hold values from 0 to 511, as said below
- edge_src: int32 [2, 65536], P(None, 'nodes'), may hold values from 0 to 1535, as said below
- edge_dst: int32 [2, 65536], P(None, 'nodes'), may hold values from 0 to 511, as said below
- edge_keep: int32 [2, 65536], P(None, 'nodes'), may hold values 0 or 1
- w_first: bfloat16 [128, 512], P(None, 'feat'), may hold values from -0.5 to 0.5
- b_first: float32 [512], P('feat'), may hold values from -3 to 3
- w_second: bfloat16 [512, 512], P(None, 'feat'), may hold values from -0.25 to 0.25
Outputs:
- normed: bfloat16 [2, 8192, 512], P(None, 'nodes', 'feat')
- correlation: float32 [512, 512], P('nodes', 'feat')
- barlow_loss: float32 [], replicated
The draws below stay inside these ranges and needn't reach their ends.
Inputs may be any that keep to these rules, and one draw needn't show every extreme that they name: `row_counts`: some partition has all 512 rows live. send_rows[i, j, h] is below row_counts[i]. `edge_src`: A source below 512 is below row_counts of the edge's partition. `edge_dst`: A partition's edge slots come in aligned blocks of 1024 slots; block k targets rows k * 128 to (k + 1) * 128 - 1.
All inputs are finite; a program needn't handle non-finite values. No bound on the sum of `edge_keep` on one device may be relied on, other than what follows from the above.
Results may differ from the reference program's by a relative error of at most 0.0017.
The reference program's roundings to bfloat16 on the way (of `hidden` and `projected`) count: a program that leaves them out, or rounds other values in their place, can miss the bound.
Values may be sent and summed in bfloat16 or wider, within the bound.
A program may use at most 64 MiB of HBM per device.

```python
import jax
import jax.numpy as jnp
from jax import lax

F_IN = 128
HID = 512
EMB = 512
ROWS_DEV = 512
HALO = 64
TILE_ROWS = 128
PARTITIONS = 16
EDGES_DEV = 4096
NODES = 8192


def shared_counts(key):
    folded = jax.random.fold_in(key, 11)
    first_key, second_key = jax.random.split(folded)
    counts = jax.random.randint(first_key, (PARTITIONS,), ROWS_DEV // 4, ROWS_DEV + 1)
    full_part = jax.random.randint(second_key, (), 0, PARTITIONS)
    return jnp.where(jnp.arange(PARTITIONS) == full_part, ROWS_DEV, counts).astype(jnp.int32)


def draw_row_counts(key, part):
    return shared_counts(key)


def draw_send_rows(key, part):
    counts = shared_counts(key)
    folded = jax.random.fold_in(key, 21)
    return jax.random.randint(folded, (PARTITIONS, PARTITIONS, HALO), 0, counts[:, None, None]).astype(jnp.int32)


def draw_edge_src(key, part):
    counts = shared_counts(key)
    folded = jax.random.fold_in(key, 31)
    local_key, remote_key, pick_key = jax.random.split(folded, 3)
    shape = (2, PARTITIONS, EDGES_DEV)
    local_src = jax.random.randint(local_key, shape, 0, counts[None, :, None])
    remote_src = ROWS_DEV + jax.random.randint(remote_key, shape, 0, PARTITIONS * HALO)
    pick = jax.random.randint(pick_key, shape, 0, 2)
    return jnp.where(pick == 1, remote_src, local_src).reshape(2, PARTITIONS * EDGES_DEV).astype(jnp.int32)


def draw_edge_dst(key, part):
    folded = jax.random.fold_in(key, 41)
    tiles = ROWS_DEV // TILE_ROWS
    shape = (2, PARTITIONS, tiles, EDGES_DEV // tiles)
    offsets = jax.random.randint(folded, shape, 0, TILE_ROWS)
    bases = (jnp.arange(tiles, dtype=jnp.int32) * TILE_ROWS)[None, None, :, None]
    return (offsets + bases).reshape(2, PARTITIONS * EDGES_DEV).astype(jnp.int32)


def plant(drawn, rng, low, top_value):
    spot = [jax.random.randint(jax.random.fold_in(rng, axis), (), 0, length) for axis, length in enumerate(drawn.shape)]
    main_axis = drawn.shape.index(max(drawn.shape))
    beside = spot[:main_axis] + [(spot[main_axis] + 1) % drawn.shape[main_axis]] + spot[main_axis + 1:]
    return drawn.at[tuple(spot)].set(low).at[tuple(beside)].set(top_value)


def shard_levels(own_key, dims, shards, least, high):
    def one(axis_at, parts):
        steps = jax.random.uniform(jax.random.fold_in(jax.random.fold_in(own_key, 6), axis_at), (parts,), jnp.float32, least / len(shards), high / len(shards))
        return jnp.repeat(jnp.exp(steps), dims[axis_at] // parts).reshape((-1,) + (1,) * (len(dims) - axis_at - 1))

    loudness = one(*shards[0])
    for cut in shards[1:]:
        loudness = loudness * one(*cut)
    return loudness


def normal_values(rng, extent, scale, reach, shards=(), kind=jnp.bfloat16):
    values = jax.random.normal(rng, extent, jnp.float32) * scale
    if len(shards) > 0:
        values = shard_levels(rng, extent, shards, -0.22, 0.18) * values
    return jnp.clip(values, min=-reach, max=reach).astype(kind)


def setup_inputs(seed: int = 0) -> dict:
    splits = jax.random.split(jax.random.key(seed), 10)
    features = normal_values(splits[0], (NODES, F_IN), 1.0, 6.0, ((0, 16),))
    row_counts = draw_row_counts(jax.random.fold_in(splits[9], 71), 0)
    send_rows = draw_send_rows(jax.random.fold_in(splits[9], 71), 0)
    edge_src = draw_edge_src(jax.random.fold_in(splits[9], 71), 0)
    edge_dst = draw_edge_dst(jax.random.fold_in(splits[9], 71), 0)
    edge_keep = plant((jax.random.randint(splits[5], (2, PARTITIONS * EDGES_DEV), 0, 4) < 3).astype(jnp.int32), jax.random.fold_in(splits[5], 1), 0, 1)
    w_first = normal_values(splits[6], (F_IN, HID), F_IN ** -0.5, 0.5, ((1, 2),))
    b_first = normal_values(splits[7], (HID,), 0.5, 3.0, ((0, 2),), jnp.float32)
    w_second = normal_values(splits[8], (HID, EMB), HID ** -0.5, 0.25, ((1, 2),))
    return {"features": features, "row_counts": row_counts, "send_rows": send_rows, "edge_src": edge_src, "edge_dst": edge_dst, "edge_keep": edge_keep, "w_first": w_first, "b_first": b_first, "w_second": w_second}


def reference(features, row_counts, send_rows, edge_src, edge_dst, edge_keep, w_first, b_first, w_second):
    partitions = row_counts.shape[0]
    local_rows = features.shape[0] // partitions
    edge_total = edge_src.shape[1] // partitions
    kept_edges = edge_keep.astype(jnp.float32)
    slot_index = jnp.arange(local_rows, dtype=jnp.int32)
    live_rows = (slot_index[None, :] < row_counts[:, None]).reshape(-1).astype(jnp.float32)[:, None]

    def mix_view(lookup, view_index):

        def per_part(part_index):
            local_block = lax.dynamic_slice_in_dim(lookup, part_index * local_rows, local_rows, 0)
            sender_base = jnp.arange(partitions, dtype=jnp.int32)[:, None] * local_rows
            inbound = (sender_base + lax.dynamic_index_in_dim(send_rows, part_index, 1, False)).reshape(-1).astype(jnp.int32)
            combined = jnp.concatenate([local_block, lookup[inbound]], 0).astype(jnp.float32)
            sources = lax.dynamic_slice_in_dim(edge_src[view_index], part_index * edge_total, edge_total, 0)
            targets = lax.dynamic_slice_in_dim(edge_dst[view_index], part_index * edge_total, edge_total, 0)
            weights = lax.dynamic_slice_in_dim(kept_edges[view_index], part_index * edge_total, edge_total, 0)
            summed = jax.ops.segment_sum(combined[sources] * weights[:, None], targets, num_segments=local_rows)
            degree = jax.ops.segment_sum(weights, targets, num_segments=local_rows)
            return (combined[:local_rows] + summed) / (1.0 + degree)[:, None]
        stacked = lax.map(per_part, jnp.arange(partitions, dtype=jnp.int32))
        return stacked.reshape(partitions * local_rows, -1)
    proj = jnp.dot(features, w_first, preferred_element_type=jnp.float32)
    live_count = jnp.sum(row_counts).astype(jnp.float32)
    normed_list = []
    for view_index in range(2):
        hidden = jax.nn.relu(mix_view(proj, view_index) + b_first).astype(jnp.bfloat16)
        projected = jnp.dot(hidden, w_second, preferred_element_type=jnp.float32).astype(jnp.bfloat16)
        embedded = mix_view(projected, view_index)
        average = lax.optimization_barrier(jnp.sum(embedded * live_rows, 0)) / live_count
        centered = (embedded - average) * live_rows
        variance = lax.optimization_barrier(jnp.sum(jnp.square(centered), 0)) / live_count
        normed_list.append((centered / jnp.sqrt(variance + 1e-05)).astype(jnp.bfloat16))
    normed = jnp.stack(normed_list)
    correlation = jnp.dot(normed[0].T, normed[1], preferred_element_type=jnp.float32) / live_count
    width = correlation.shape[0]
    diagonal = jnp.arange(width, dtype=jnp.int32)[:, None] == jnp.arange(width, dtype=jnp.int32)[None, :]
    barlow_loss = jnp.sum(jnp.where(diagonal, jnp.square(1.0 - correlation), 0.005 * jnp.square(correlation)))
    return (normed, correlation, barlow_loss)
```

```python
import functools

import jax
import jax.numpy as jnp
from jax import lax
from jax.experimental import pallas as pl
from jax.experimental.pallas import tpu as pltpu
from jax.sharding import PartitionSpec as P

MESH = pl.DeviceIdType.MESH
F32 = jnp.float32
BF16 = jnp.bfloat16
TILE = 128


def dot(a, b):
    return jnp.dot(a, b, preferred_element_type=F32)


def kernel(
    parts, feats,
    feat_ref, count_ref, send_ref, src_ref, dst_ref, keep_ref, wf_ref, bf_ref, ws_ref,
    normed_ref, corr_ref, loss_ref,
    pad, pick, gath1, tab1, gath2, tab2, a_hi, a_lo, deg, wf_all, bf_all, ws_all, hid, acc,
    st_own, st_all, mine, other, p_send, p_recv, l_own, l_all,
    send_sem, recv_sem, w_send, w_recv, n_send, n_recv,
):
    me = lax.axis_index("nodes")
    core = lax.axis_index("feat")
    mate = 1 - core
    rows, width = feat_ref.shape
    halo = send_ref.shape[2]
    emb = hid.shape[1]
    half = ws_ref.shape[1]
    tiles = rows // TILE
    per_tile = src_ref.shape[1] // tiles
    sources = tab1.shape[0]
    share = p_send.shape[1]
    others = parts - 1

    def peer(offset):
        return lax.rem(me + offset, parts)

    def each(fn):
        def body(offset, carry):
            fn(peer(offset))
            return carry
        lax.fori_loop(1, parts, body, 0)

    barrier = pltpu.get_barrier_semaphore()

    def greet(offset, carry):
        to = peer(offset)
        pl.semaphore_signal(barrier, inc=1, device_id={"nodes": to, "feat": core}, device_id_type=MESH)
        pl.semaphore_signal(barrier, inc=1, device_id={"nodes": to, "feat": mate}, device_id_type=MESH)
        return carry

    lax.fori_loop(1, parts, greet, 0)
    pl.semaphore_signal(barrier, inc=1, device_id={"nodes": me, "feat": mate}, device_id_type=MESH)

    pad[...] = jnp.zeros_like(pad)
    pad[0:parts, 0:halo] = send_ref[0].astype(F32)
    turned = pad[...].T
    lanes = lax.broadcasted_iota(jnp.int32, (halo, rows), 1).astype(F32)
    for p in range(parts):
        hot = turned[0:halo, p:p + 1] == lanes
        pick[p * halo:(p + 1) * halo, :] = jnp.where(hot, 1.0, 0.0).astype(BF16)
    tab1[0:rows, :] = feat_ref[...]
    out_rows = parts * halo
    step_rows = min(512, out_rows)

    def gather(table, dst):
        def body(c, carry):
            at = pl.ds(pl.multiple_of(c * step_rows, step_rows), step_rows)
            dst[at, :] = dot(pick[at, :], table()).astype(BF16)
            return carry
        lax.fori_loop(0, out_rows // step_rows, body, 0)

    gather(lambda: feat_ref[...], gath1)

    pl.semaphore_wait(barrier, parts * feats - 1)

    def slot(p):
        return pl.ds(pl.multiple_of(p * halo, halo), halo)

    def landing(p):
        return pl.ds(pl.multiple_of(rows + p * halo, halo), halo)

    def remote(src, dst, ssem, rsem, to, c):
        return pltpu.make_async_remote_copy(
            src_ref=src, dst_ref=dst, send_sem=ssem, recv_sem=rsem,
            device_id={"nodes": to, "feat": c}, device_id_type=MESH,
        )

    def drain(ref, sem):
        pltpu.make_async_copy(ref, ref, sem).wait()

    each(lambda to: remote(
        gath1.at[slot(to)], tab1.at[landing(me)], send_sem.at[0], recv_sem.at[0], to, core).start())
    weights = [
        remote(wf_ref, wf_all.at[core], w_send.at[0], w_recv.at[0], me, mate),
        remote(bf_ref, bf_all.at[core], w_send.at[1], w_recv.at[1], me, mate),
        remote(ws_ref, ws_all.at[core], w_send.at[2], w_recv.at[2], me, mate),
    ]
    for copy in weights:
        copy.start()
    wf_all[core] = wf_ref[...]
    bf_all[core] = bf_ref[...]
    ws_all[core] = ws_ref[...]
    tab1[landing(me), :] = gath1[slot(me), :]

    chunk = 256
    first_view = core == 0

    def view_row(ref, k):
        at = pl.ds(pl.multiple_of(k * per_tile, per_tile), per_tile)
        return jnp.where(first_view, ref[0:1, at], ref[1:2, at])

    def count_tile(k, carry):
        src = view_row(src_ref, k)
        dst = jnp.where(view_row(keep_ref, k) == 1, view_row(dst_ref, k) - k * TILE, -1)
        row_at = lax.broadcasted_iota(jnp.int32, (TILE, per_tile), 0)
        hits = jnp.where(row_at == dst, 1.0, 0.0)
        at = pl.ds(pl.multiple_of(k * TILE, TILE), TILE)
        deg[at, :] = 1.0 / (1.0 + jnp.sum(hits, axis=1, keepdims=True))
        hits = hits.astype(BF16)

        def count_chunk(c, inner):
            source_at = lax.broadcasted_iota(jnp.int32, (chunk, per_tile), 0)
            hot = jnp.where(source_at == src - c * chunk, 1.0, 0.0).astype(BF16)
            counts = lax.dot_general(hits, hot, (((1,), (1,)), ((), ())), preferred_element_type=F32)
            self_row = lax.broadcasted_iota(jnp.int32, (TILE, chunk), 0) + k * TILE
            self_col = lax.broadcasted_iota(jnp.int32, (TILE, chunk), 1) + c * chunk
            counts = counts + jnp.where(self_row == self_col, 1.0, 0.0)
            high = counts.astype(BF16)
            cols = pl.ds(pl.multiple_of(c * chunk, chunk), chunk)
            a_hi[at, cols] = high
            a_lo[at, cols] = (counts - high.astype(F32)).astype(BF16)
            return inner

        lax.fori_loop(0, sources // chunk, count_chunk, 0)
        return carry

    lax.fori_loop(0, tiles, count_tile, 0)

    depth = 512 if sources % 512 == 0 else 256

    def mixed(table, c):
        cols = pl.ds(pl.multiple_of(c * depth, depth), depth)
        part = table[cols, :]
        return dot(a_hi[:, cols], part) + dot(a_lo[:, cols], part)

    drain(tab1.at[pl.ds(rows, others * halo)], recv_sem.at[0])
    summed = lax.fori_loop(
        0, sources // depth, lambda c, total: total + mixed(tab1, c), jnp.zeros((rows, width), F32))
    part0 = summed.astype(BF16)
    rest = summed - part0.astype(F32)
    part1 = rest.astype(BF16)
    part2 = (rest - part1.astype(F32)).astype(BF16)
    for copy in weights:
        copy.wait_recv()
    for h in range(feats):
        w = wf_all[h]
        proj = dot(part0, w) + (dot(part1, w) + dot(part2, w))
        hid[:, h * half:(h + 1) * half] = jnp.maximum(proj * deg[...] + bf_all[h], 0.0).astype(BF16)
    for h in range(feats):
        tab2[0:rows, h * half:(h + 1) * half] = dot(hid[...], ws_all[h]).astype(BF16)

    gather(lambda: tab2[0:rows, :], gath2)
    each(lambda to: remote(
        gath2.at[slot(to)], tab2.at[landing(me)], send_sem.at[1], recv_sem.at[1], to, core).start())
    tab2[landing(me), :] = gath2[slot(me), :]
    local = rows // depth
    acc[...] = mixed(tab2, 0)
    for c in range(1, local):
        acc[...] += mixed(tab2, c)
    drain(tab2.at[pl.ds(rows, others * halo)], recv_sem.at[1])

    def add_chunk(c, carry):
        acc[...] += mixed(tab2, c)
        return carry

    lax.fori_loop(local, sources // depth, add_chunk, 0)

    live_count = count_ref[0]
    live = lax.broadcasted_iota(jnp.int32, (rows, 1), 0) < live_count
    mine_count = live_count.astype(F32)
    blocks = emb // TILE
    for q in range(blocks):
        cols = slice(q * TILE, (q + 1) * TILE)
        value = acc[:, cols] * deg[...]
        acc[:, cols] = value
        total = jnp.sum(jnp.where(live, value, 0.0), axis=0, keepdims=True)
        off = jnp.where(live, value - total / mine_count, 0.0)
        st_own[q:q + 1, :] = total
        st_own[blocks + q:blocks + q + 1, :] = jnp.sum(off * off, axis=0, keepdims=True)
    tail = st_own.shape[0] - 2 * blocks
    st_own[2 * blocks:, :] = jnp.zeros((tail, TILE), F32) + mine_count
    each(lambda to: remote(
        st_own, st_all.at[me], send_sem.at[2], recv_sem.at[2], to, core).start())
    st_all[me] = st_own[...]
    drain(st_all.at[pl.ds(0, others)], recv_sem.at[2])
    sizes = st_all[:, 2 * blocks:2 * blocks + 1, :]
    sums = st_all[:, 0:blocks, :]
    spreads = st_all[:, blocks:2 * blocks, :]
    node_total = jnp.sum(sizes, axis=0)
    average = jnp.sum(sums, axis=0) / node_total
    shift = sums / sizes - average[None]
    variance = jnp.sum(spreads + sizes * shift * shift, axis=0) / node_total
    scale = 1.0 / jnp.sqrt(variance + 1e-05)
    for q in range(blocks):
        value = (acc[:, q * TILE:(q + 1) * TILE] - average[q:q + 1, :]) * scale[q:q + 1, :]
        per_half = half // TILE
        at = (q % per_half) * TILE
        mine[q // per_half, :, at:at + TILE] = jnp.where(live, value, 0.0).astype(BF16)

    swap = remote(mine.at[mate], other.at[mate], n_send.at[0], n_recv.at[0], me, mate)
    extra = remote(mine.at[core], other.at[core], n_send.at[1], n_recv.at[1], me, mate)
    swap.start()

    @pl.when(first_view)
    def _():
        extra.start()

    normed_ref[core] = mine[core]
    contract = (((0,), (0,)), ((), ()))

    def put(h, product):
        per = half // share
        for j in range(per):
            p_send[h * per + j] = product[j * share:(j + 1) * share, :]

    swap.wait_recv()
    normed_ref[mate] = other[core]

    @pl.when(first_view)
    def _():
        for h in range(feats):
            put(h, lax.dot_general(mine[h], other[0], contract, preferred_element_type=F32))

    @pl.when(jnp.logical_not(first_view))
    def _():
        put(1, lax.dot_general(other[1], mine[1], contract, preferred_element_type=F32))
        pltpu.make_async_copy(other.at[0], other.at[0], n_recv.at[1]).wait()
        put(0, lax.dot_general(other[0], mine[1], contract, preferred_element_type=F32))

    each(lambda to: remote(
        p_send.at[to], p_recv.at[me], send_sem.at[3], recv_sem.at[3], to, core).start())
    p_recv[me] = p_send[me]
    drain(p_recv.at[pl.ds(0, others)], recv_sem.at[3])
    total = node_total[:, 0:1]
    corr = jnp.sum(p_recv[...], axis=0) / total
    corr_ref[...] = corr
    row_label = lax.broadcasted_iota(jnp.int32, (share, half), 0) + me * share
    col_label = lax.broadcasted_iota(jnp.int32, (share, half), 1) + core * half
    miss = 1.0 - corr
    terms = jnp.where(row_label == col_label, miss * miss, 0.005 * (corr * corr))
    line = jnp.sum(terms, axis=0, keepdims=True)
    folded = line[:, 0:TILE]
    for q in range(1, half // TILE):
        folded = folded + line[:, q * TILE:(q + 1) * TILE]
    l_own[...] = folded
    spot = me * feats + core

    def tell(offset, carry):
        to = peer(offset)
        remote(l_own, l_all.at[spot], send_sem.at[4], recv_sem.at[4], to, core).start()
        remote(l_own, l_all.at[spot], send_sem.at[4], recv_sem.at[4], to, mate).start()
        return carry

    lax.fori_loop(1, parts, tell, 0)
    remote(l_own, l_all.at[spot], send_sem.at[4], recv_sem.at[4], me, mate).start()
    l_all[spot] = folded
    drain(l_all.at[pl.ds(0, parts * feats - 1)], recv_sem.at[4])
    loss_ref[0, 0] = jnp.sum(l_all[...])

    for copy in weights:
        copy.wait_send()
    swap.wait_send()

    @pl.when(first_view)
    def _():
        extra.wait_send()

    drain(gath1.at[pl.ds(0, others * halo)], send_sem.at[0])
    drain(gath2.at[pl.ds(0, others * halo)], send_sem.at[1])
    drain(st_all.at[pl.ds(0, others)], send_sem.at[2])
    drain(p_send.at[pl.ds(0, others)], send_sem.at[3])
    drain(l_all.at[pl.ds(0, parts * feats - 1)], send_sem.at[4])


def per_device(
    features, row_counts, send_rows, edge_src, edge_dst, edge_keep, w_first, b_first, w_second
):
    parts = lax.axis_size("nodes")
    feats = lax.axis_size("feat")
    rows, width = features.shape
    halo = send_rows.shape[2]
    half = w_first.shape[1]
    hidden, emb_half = w_second.shape
    emb = emb_half * feats
    share = emb // parts
    sources = rows + parts * halo
    blocks = emb // TILE
    vmem = pl.BlockSpec(memory_space=pltpu.VMEM)
    smem = pl.BlockSpec(memory_space=pltpu.SMEM)
    pad_rows = -(-parts // TILE) * TILE
    normed, correlation, loss = pl.pallas_call(
        functools.partial(kernel, parts, feats),
        out_shape=(
            jax.ShapeDtypeStruct((2, rows, emb_half), BF16),
            jax.ShapeDtypeStruct((share, emb_half), F32),
            jax.ShapeDtypeStruct((1, 1), F32),
        ),
        in_specs=[vmem, smem] + [vmem] * 7,
        out_specs=(vmem, vmem, smem),
        scratch_shapes=[
            pltpu.VMEM((pad_rows, TILE), F32),
            pltpu.VMEM((parts * halo, rows), BF16),
            pltpu.VMEM((parts * halo, width), BF16),
            pltpu.VMEM((sources, width), BF16),
            pltpu.VMEM((parts * halo, emb), BF16),
            pltpu.VMEM((sources, emb), BF16),
            pltpu.VMEM((rows, sources), BF16),
            pltpu.VMEM((rows, sources), BF16),
            pltpu.VMEM((rows, 1), F32),
            pltpu.VMEM((feats, width, half), BF16),
            pltpu.VMEM((feats, 1, half), F32),
            pltpu.VMEM((feats, hidden, emb_half), BF16),
            pltpu.VMEM((rows, hidden), BF16),
            pltpu.VMEM((rows, emb), F32),
            pltpu.VMEM((2 * blocks + 8, TILE), F32),
            pltpu.VMEM((parts, 2 * blocks + 8, TILE), F32),
            pltpu.VMEM((feats, rows, emb_half), BF16),
            pltpu.VMEM((feats, rows, emb_half), BF16),
            pltpu.VMEM((parts, share, emb_half), F32),
            pltpu.VMEM((parts, share, emb_half), F32),
            pltpu.VMEM((1, TILE), F32),
            pltpu.VMEM((parts * feats, 1, TILE), F32),
            pltpu.SemaphoreType.DMA((5,)),
            pltpu.SemaphoreType.DMA((5,)),
            pltpu.SemaphoreType.DMA((3,)),
            pltpu.SemaphoreType.DMA((3,)),
            pltpu.SemaphoreType.DMA((2,)),
            pltpu.SemaphoreType.DMA((2,)),
        ],
        compiler_params=pltpu.CompilerParams(
            collective_id=0, has_side_effects=True, vmem_limit_bytes=60 * 1024 * 1024
        ),
    )(
        features, row_counts, send_rows, edge_src, edge_dst, edge_keep, w_first,
        b_first.reshape(1, half), w_second,
    )
    return normed, correlation, loss.reshape(())


def solution(mesh):
    placed = (
        P("nodes", None),
        P("nodes"),
        P("nodes", None, None),
        P(None, "nodes"),
        P(None, "nodes"),
        P(None, "nodes"),
        P(None, "feat"),
        P("feat"),
        P(None, "feat"),
    )
    return jax.shard_map(
        per_device,
        mesh=mesh,
        in_specs=placed,
        out_specs=(P(None, "nodes", "feat"), P("nodes", "feat"), P()),
        check_vma=False,
    )
```

```python
import functools

import jax
import jax.numpy as jnp
from jax import lax
from jax.experimental import pallas as pl
from jax.experimental.pallas import tpu as pltpu
from jax.sharding import PartitionSpec as P

MESH = pl.DeviceIdType.MESH
F32 = jnp.float32
BF16 = jnp.bfloat16
TILE = 128


def dot(a, b):
    return jnp.dot(a, b, preferred_element_type=F32)


def split(value, count):
    found = []
    for _ in range(count - 1):
        found.append(value.astype(BF16))
        value = value - found[-1].astype(F32)
    return found + [value.astype(BF16)]


def kernel(
    parts, feats,
    feat_ref, count_ref, send_ref, src_ref, dst_ref, keep_ref, wf_ref, bf_ref, ws_ref,
    normed_ref, corr_ref, loss_ref,
    pad, pick, gath1, tab1, gath2, tabm, tab2, a_hi, a_lo, deg, wf_all, bf_all, ws_all, hid, acc,
    st_own, st_all, mine, other, p_send, p_recv, l_own, l_all,
    send_sem, recv_sem, w_send, w_recv, n_send, n_recv,
):
    me = lax.axis_index("nodes")
    core = lax.axis_index("feat")
    mate = 1 - core
    rows, width = feat_ref.shape
    halo = send_ref.shape[2]
    emb = hid.shape[1]
    half = ws_ref.shape[1]
    tiles = rows // TILE
    per_tile = src_ref.shape[1] // tiles
    sources = tab1.shape[0]
    share = p_send.shape[1]
    others = parts - 1

    def peer(offset):
        return lax.rem(me + offset, parts)

    def each(fn):
        def body(offset, carry):
            fn(peer(offset))
            return carry
        lax.fori_loop(1, parts, body, 0)

    barrier = pltpu.get_barrier_semaphore()

    def greet(offset, carry):
        to = peer(offset)
        pl.semaphore_signal(barrier, inc=1, device_id={"nodes": to, "feat": core}, device_id_type=MESH)
        pl.semaphore_signal(barrier, inc=1, device_id={"nodes": to, "feat": mate}, device_id_type=MESH)
        return carry

    lax.fori_loop(1, parts, greet, 0)
    pl.semaphore_signal(barrier, inc=1, device_id={"nodes": me, "feat": mate}, device_id_type=MESH)

    pad[...] = jnp.zeros_like(pad)
    pad[0:parts, 0:halo] = send_ref[0].astype(F32)
    turned = pad[...].T
    lanes = lax.broadcasted_iota(jnp.int32, (halo, rows), 1).astype(F32)
    for p in range(parts):
        hot = turned[0:halo, p:p + 1] == lanes
        pick[p * halo:(p + 1) * halo, :] = jnp.where(hot, 1.0, 0.0).astype(BF16)
    tab1[0:rows, :] = feat_ref[...]
    out_rows = parts * halo
    step_rows = min(512, out_rows)

    def gather(table, dst):
        def body(c, carry):
            at = pl.ds(pl.multiple_of(c * step_rows, step_rows), step_rows)
            dst[at, :] = dot(pick[at, :], table()).astype(BF16)
            return carry
        lax.fori_loop(0, out_rows // step_rows, body, 0)

    gather(lambda: feat_ref[...], gath1)

    pl.semaphore_wait(barrier, parts * feats - 1)

    def slot(p):
        return pl.ds(pl.multiple_of(p * halo, halo), halo)

    def landing(p):
        return pl.ds(pl.multiple_of(rows + p * halo, halo), halo)

    def remote(src, dst, ssem, rsem, to, c):
        return pltpu.make_async_remote_copy(
            src_ref=src, dst_ref=dst, send_sem=ssem, recv_sem=rsem,
            device_id={"nodes": to, "feat": c}, device_id_type=MESH,
        )

    def drain(ref, sem):
        pltpu.make_async_copy(ref, ref, sem).wait()

    each(lambda to: remote(
        gath1.at[slot(to)], tab1.at[landing(me)], send_sem.at[0], recv_sem.at[0], to, core).start())
    weights = [
        remote(wf_ref, wf_all.at[core], w_send.at[0], w_recv.at[0], me, mate),
        remote(bf_ref, bf_all.at[core], w_send.at[1], w_recv.at[1], me, mate),
        remote(ws_ref, ws_all.at[core], w_send.at[2], w_recv.at[2], me, mate),
    ]
    for copy in weights:
        copy.start()
    wf_all[core] = wf_ref[...]
    bf_all[core] = bf_ref[...]
    ws_all[core] = ws_ref[...]
    tab1[landing(me), :] = gath1[slot(me), :]

    chunk = 256
    first_view = core == 0

    def view_row(ref, k):
        at = pl.ds(pl.multiple_of(k * per_tile, per_tile), per_tile)
        return jnp.where(first_view, ref[0:1, at], ref[1:2, at])

    def count_tile(k, carry):
        src = view_row(src_ref, k)
        dst = jnp.where(view_row(keep_ref, k) == 1, view_row(dst_ref, k) - k * TILE, -1)
        row_at = lax.broadcasted_iota(jnp.int32, (TILE, per_tile), 0)
        hits = jnp.where(row_at == dst, 1.0, 0.0)
        at = pl.ds(pl.multiple_of(k * TILE, TILE), TILE)
        deg[at, :] = 1.0 / (1.0 + jnp.sum(hits, axis=1, keepdims=True))
        hits = hits.astype(BF16)

        def count_chunk(c, inner):
            source_at = lax.broadcasted_iota(jnp.int32, (chunk, per_tile), 0)
            hot = jnp.where(source_at == src - c * chunk, 1.0, 0.0).astype(BF16)
            counts = lax.dot_general(hits, hot, (((1,), (1,)), ((), ())), preferred_element_type=F32)
            self_row = lax.broadcasted_iota(jnp.int32, (TILE, chunk), 0) + k * TILE
            self_col = lax.broadcasted_iota(jnp.int32, (TILE, chunk), 1) + c * chunk
            counts = counts + jnp.where(self_row == self_col, 1.0, 0.0)
            high = counts.astype(BF16)
            cols = pl.ds(pl.multiple_of(c * chunk, chunk), chunk)
            a_hi[at, cols] = high
            a_lo[at, cols] = (counts - high.astype(F32)).astype(BF16)
            return inner

        lax.fori_loop(0, sources // chunk, count_chunk, 0)
        return carry

    lax.fori_loop(0, tiles, count_tile, 0)

    depth = 512 if sources % 512 == 0 else 256

    def mixed(table, c):
        cols = pl.ds(pl.multiple_of(c * depth, depth), depth)
        part = table[cols, :]
        return dot(a_hi[:, cols], part) + dot(a_lo[:, cols], part)

    drain(tab1.at[pl.ds(rows, others * halo)], recv_sem.at[0])
    summed = lax.fori_loop(
        0, sources // depth, lambda c, total: total + mixed(tab1, c), jnp.zeros((rows, width), F32))
    mean = summed * deg[...]
    tabm[0:rows, :] = mean
    parts3 = split(mean, 3)

    def gather_mean(c, carry):
        at = pl.ds(pl.multiple_of(c * step_rows, step_rows), step_rows)
        hot = pick[at, :]
        gath2[at, :] = dot(hot, parts3[0]) + (dot(hot, parts3[1]) + dot(hot, parts3[2]))
        return carry

    lax.fori_loop(0, out_rows // step_rows, gather_mean, 0)
    each(lambda to: remote(
        gath2.at[slot(to)], tabm.at[landing(me)], send_sem.at[1], recv_sem.at[1], to, core).start())
    tabm[landing(me), :] = gath2[slot(me), :]
    for copy in weights:
        copy.wait_recv()

    def rows_of(c):
        at = pl.ds(pl.multiple_of(c * depth, depth), depth)
        wide = jnp.concatenate(split(tabm[at, :], 2), axis=1)
        for h in range(feats):
            w = wf_all[h]
            proj = dot(wide, jnp.concatenate([w, w], axis=0))
            hid[:, h * half:(h + 1) * half] = jnp.maximum(proj + bf_all[h], 0.0).astype(BF16)
        for h in range(feats):
            tab2[at, h * half:(h + 1) * half] = dot(hid[...], ws_all[h]).astype(BF16)

    local = rows // depth
    for c in range(local):
        rows_of(c)
        if c == 0:
            acc[...] = mixed(tab2, c)
        else:
            acc[...] += mixed(tab2, c)
    drain(tabm.at[pl.ds(rows, others * halo)], recv_sem.at[1])

    def add_chunk(c, carry):
        rows_of(c)
        acc[...] += mixed(tab2, c)
        return carry

    lax.fori_loop(local, sources // depth, add_chunk, 0)

    live_count = count_ref[0]
    live = lax.broadcasted_iota(jnp.int32, (rows, 1), 0) < live_count
    mine_count = live_count.astype(F32)
    blocks = emb // TILE
    for q in range(blocks):
        cols = slice(q * TILE, (q + 1) * TILE)
        value = acc[:, cols] * deg[...]
        acc[:, cols] = value
        total = jnp.sum(jnp.where(live, value, 0.0), axis=0, keepdims=True)
        off = jnp.where(live, value - total / mine_count, 0.0)
        st_own[q:q + 1, :] = total
        st_own[blocks + q:blocks + q + 1, :] = jnp.sum(off * off, axis=0, keepdims=True)
    tail = st_own.shape[0] - 2 * blocks
    st_own[2 * blocks:, :] = jnp.zeros((tail, TILE), F32) + mine_count
    each(lambda to: remote(
        st_own, st_all.at[me], send_sem.at[2], recv_sem.at[2], to, core).start())
    st_all[me] = st_own[...]
    drain(st_all.at[pl.ds(0, others)], recv_sem.at[2])
    sizes = st_all[:, 2 * blocks:2 * blocks + 1, :]
    sums = st_all[:, 0:blocks, :]
    spreads = st_all[:, blocks:2 * blocks, :]
    node_total = jnp.sum(sizes, axis=0)
    average = jnp.sum(sums, axis=0) / node_total
    shift = sums / sizes - average[None]
    variance = jnp.sum(spreads + sizes * shift * shift, axis=0) / node_total
    scale = 1.0 / jnp.sqrt(variance + 1e-05)
    for q in range(blocks):
        value = (acc[:, q * TILE:(q + 1) * TILE] - average[q:q + 1, :]) * scale[q:q + 1, :]
        per_half = half // TILE
        at = (q % per_half) * TILE
        mine[q // per_half, :, at:at + TILE] = jnp.where(live, value, 0.0).astype(BF16)

    swap = remote(mine.at[mate], other.at[mate], n_send.at[0], n_recv.at[0], me, mate)
    extra = remote(mine.at[core], other.at[core], n_send.at[1], n_recv.at[1], me, mate)
    swap.start()

    @pl.when(first_view)
    def _():
        extra.start()

    normed_ref[core] = mine[core]
    contract = (((0,), (0,)), ((), ()))

    def put(h, product):
        per = half // share
        for j in range(per):
            p_send[h * per + j] = product[j * share:(j + 1) * share, :]

    swap.wait_recv()
    normed_ref[mate] = other[core]

    @pl.when(first_view)
    def _():
        for h in range(feats):
            put(h, lax.dot_general(mine[h], other[0], contract, preferred_element_type=F32))

    @pl.when(jnp.logical_not(first_view))
    def _():
        put(1, lax.dot_general(other[1], mine[1], contract, preferred_element_type=F32))
        pltpu.make_async_copy(other.at[0], other.at[0], n_recv.at[1]).wait()
        put(0, lax.dot_general(other[0], mine[1], contract, preferred_element_type=F32))

    each(lambda to: remote(
        p_send.at[to], p_recv.at[me], send_sem.at[3], recv_sem.at[3], to, core).start())
    p_recv[me] = p_send[me]
    drain(p_recv.at[pl.ds(0, others)], recv_sem.at[3])
    total = node_total[:, 0:1]
    corr = jnp.sum(p_recv[...], axis=0) / total
    corr_ref[...] = corr
    row_label = lax.broadcasted_iota(jnp.int32, (share, half), 0) + me * share
    col_label = lax.broadcasted_iota(jnp.int32, (share, half), 1) + core * half
    miss = 1.0 - corr
    terms = jnp.where(row_label == col_label, miss * miss, 0.005 * (corr * corr))
    line = jnp.sum(terms, axis=0, keepdims=True)
    folded = line[:, 0:TILE]
    for q in range(1, half // TILE):
        folded = folded + line[:, q * TILE:(q + 1) * TILE]
    l_own[...] = folded
    spot = me * feats + core

    def tell(offset, carry):
        to = peer(offset)
        remote(l_own, l_all.at[spot], send_sem.at[4], recv_sem.at[4], to, core).start()
        remote(l_own, l_all.at[spot], send_sem.at[4], recv_sem.at[4], to, mate).start()
        return carry

    lax.fori_loop(1, parts, tell, 0)
    remote(l_own, l_all.at[spot], send_sem.at[4], recv_sem.at[4], me, mate).start()
    l_all[spot] = folded
    drain(l_all.at[pl.ds(0, parts * feats - 1)], recv_sem.at[4])
    loss_ref[0, 0] = jnp.sum(l_all[...])

    for copy in weights:
        copy.wait_send()
    swap.wait_send()

    @pl.when(first_view)
    def _():
        extra.wait_send()

    drain(gath1.at[pl.ds(0, others * halo)], send_sem.at[0])
    drain(gath2.at[pl.ds(0, others * halo)], send_sem.at[1])
    drain(st_all.at[pl.ds(0, others)], send_sem.at[2])
    drain(p_send.at[pl.ds(0, others)], send_sem.at[3])
    drain(l_all.at[pl.ds(0, parts * feats - 1)], send_sem.at[4])


def per_device(
    features, row_counts, send_rows, edge_src, edge_dst, edge_keep, w_first, b_first, w_second
):
    parts = lax.axis_size("nodes")
    feats = lax.axis_size("feat")
    rows, width = features.shape
    halo = send_rows.shape[2]
    half = w_first.shape[1]
    hidden, emb_half = w_second.shape
    emb = emb_half * feats
    share = emb // parts
    sources = rows + parts * halo
    blocks = emb // TILE
    vmem = pl.BlockSpec(memory_space=pltpu.VMEM)
    smem = pl.BlockSpec(memory_space=pltpu.SMEM)
    pad_rows = -(-parts // TILE) * TILE
    normed, correlation, loss = pl.pallas_call(
        functools.partial(kernel, parts, feats),
        out_shape=(
            jax.ShapeDtypeStruct((2, rows, emb_half), BF16),
            jax.ShapeDtypeStruct((share, emb_half), F32),
            jax.ShapeDtypeStruct((1, 1), F32),
        ),
        in_specs=[vmem, smem] + [vmem] * 7,
        out_specs=(vmem, vmem, smem),
        scratch_shapes=[
            pltpu.VMEM((pad_rows, TILE), F32),
            pltpu.VMEM((parts * halo, rows), BF16),
            pltpu.VMEM((parts * halo, width), BF16),
            pltpu.VMEM((sources, width), BF16),
            pltpu.VMEM((parts * halo, width), F32),
            pltpu.VMEM((sources, width), F32),
            pltpu.VMEM((sources, emb), BF16),
            pltpu.VMEM((rows, sources), BF16),
            pltpu.VMEM((rows, sources), BF16),
            pltpu.VMEM((rows, 1), F32),
            pltpu.VMEM((feats, width, half), BF16),
            pltpu.VMEM((feats, 1, half), F32),
            pltpu.VMEM((feats, hidden, emb_half), BF16),
            pltpu.VMEM((512 if sources % 512 == 0 else 256, hidden), BF16),
            pltpu.VMEM((rows, emb), F32),
            pltpu.VMEM((2 * blocks + 8, TILE), F32),
            pltpu.VMEM((parts, 2 * blocks + 8, TILE), F32),
            pltpu.VMEM((feats, rows, emb_half), BF16),
            pltpu.VMEM((feats, rows, emb_half), BF16),
            pltpu.VMEM((parts, share, emb_half), F32),
            pltpu.VMEM((parts, share, emb_half), F32),
            pltpu.VMEM((1, TILE), F32),
            pltpu.VMEM((parts * feats, 1, TILE), F32),
            pltpu.SemaphoreType.DMA((5,)),
            pltpu.SemaphoreType.DMA((5,)),
            pltpu.SemaphoreType.DMA((3,)),
            pltpu.SemaphoreType.DMA((3,)),
            pltpu.SemaphoreType.DMA((2,)),
            pltpu.SemaphoreType.DMA((2,)),
        ],
        compiler_params=pltpu.CompilerParams(
            collective_id=0, has_side_effects=True, vmem_limit_bytes=60 * 1024 * 1024
        ),
    )(
        features, row_counts, send_rows, edge_src, edge_dst, edge_keep, w_first,
        b_first.reshape(1, half), w_second,
    )
    return normed, correlation, loss.reshape(())


def solution(mesh):
    placed = (
        P("nodes", None),
        P("nodes"),
        P("nodes", None, None),
        P(None, "nodes"),
        P(None, "nodes"),
        P(None, "nodes"),
        P(None, "feat"),
        P("feat"),
        P(None, "feat"),
    )
    return jax.shard_map(
        per_device,
        mesh=mesh,
        in_specs=placed,
        out_specs=(P(None, "nodes", "feat"), P("nodes", "feat"), P()),
        check_vma=False,
    )
```

```python
import functools

import jax
import jax.numpy as jnp
from jax import lax
from jax.experimental import pallas as pl
from jax.experimental.pallas import tpu as pltpu
from jax.sharding import PartitionSpec as P

MESH = pl.DeviceIdType.MESH
F32 = jnp.float32
BF16 = jnp.bfloat16
TILE = 128


def dot(a, b):
    return jnp.dot(a, b, preferred_element_type=F32)


def split(value, count):
    found = []
    for _ in range(count - 1):
        found.append(value.astype(BF16))
        value = value - found[-1].astype(F32)
    return found + [value.astype(BF16)]


def kernel(
    parts, feats,
    feat_ref, count_ref, send_ref, src_ref, dst_ref, keep_ref, wf_ref, bf_ref, ws_ref,
    normed_ref, corr_ref, loss_ref,
    pad, pick, gath1, tab1, gath2, tabm, tab2, a_hi, a_lo, deg, wf_all, bf_all, ws_all, hid, acc,
    st_own, st_all, mine, other, p_send, p_recv, l_own, l_mate, l_sum, l_all,
    send_sem, recv_sem, w_send, w_recv, n_send, n_recv,
):
    me = lax.axis_index("nodes")
    core = lax.axis_index("feat")
    mate = 1 - core
    rows, width = feat_ref.shape
    halo = send_ref.shape[2]
    emb = hid.shape[1]
    half = ws_ref.shape[1]
    tiles = rows // TILE
    per_tile = src_ref.shape[1] // tiles
    sources = tab1.shape[0]
    share = p_send.shape[1]
    others = parts - 1

    def peer(offset):
        return lax.rem(me + offset, parts)

    def each(fn):
        def body(offset, carry):
            fn(peer(offset))
            return carry
        lax.fori_loop(1, parts, body, 0)

    barrier = pltpu.get_barrier_semaphore()

    def greet(offset, carry):
        to = peer(offset)
        pl.semaphore_signal(barrier, inc=1, device_id={"nodes": to, "feat": core}, device_id_type=MESH)
        pl.semaphore_signal(barrier, inc=1, device_id={"nodes": to, "feat": mate}, device_id_type=MESH)
        return carry

    lax.fori_loop(1, parts, greet, 0)
    pl.semaphore_signal(barrier, inc=1, device_id={"nodes": me, "feat": mate}, device_id_type=MESH)

    pad[...] = jnp.zeros_like(pad)
    pad[0:parts, 0:halo] = send_ref[0].astype(F32)
    turned = pad[...].T
    lanes = lax.broadcasted_iota(jnp.int32, (halo, rows), 1).astype(F32)
    for p in range(parts):
        hot = turned[0:halo, p:p + 1] == lanes
        pick[p * halo:(p + 1) * halo, :] = jnp.where(hot, 1.0, 0.0).astype(BF16)
    tab1[0:rows, :] = feat_ref[...]
    out_rows = parts * halo
    step_rows = min(512, out_rows)

    def gather(table, dst):
        def body(c, carry):
            at = pl.ds(pl.multiple_of(c * step_rows, step_rows), step_rows)
            dst[at, :] = dot(pick[at, :], table()).astype(BF16)
            return carry
        lax.fori_loop(0, out_rows // step_rows, body, 0)

    gather(lambda: feat_ref[...], gath1)

    pl.semaphore_wait(barrier, parts * feats - 1)

    def slot(p):
        return pl.ds(pl.multiple_of(p * halo, halo), halo)

    def landing(p):
        return pl.ds(pl.multiple_of(rows + p * halo, halo), halo)

    def remote(src, dst, ssem, rsem, to, c):
        return pltpu.make_async_remote_copy(
            src_ref=src, dst_ref=dst, send_sem=ssem, recv_sem=rsem,
            device_id={"nodes": to, "feat": c}, device_id_type=MESH,
        )

    def drain(ref, sem):
        pltpu.make_async_copy(ref, ref, sem).wait()

    each(lambda to: remote(
        gath1.at[slot(to)], tab1.at[landing(me)], send_sem.at[0], recv_sem.at[0], to, core).start())
    weights = [
        remote(wf_ref, wf_all.at[core], w_send.at[0], w_recv.at[0], me, mate),
        remote(bf_ref, bf_all.at[core], w_send.at[1], w_recv.at[1], me, mate),
        remote(ws_ref, ws_all.at[core], w_send.at[2], w_recv.at[2], me, mate),
    ]
    for copy in weights:
        copy.start()
    wf_all[core] = wf_ref[...]
    bf_all[core] = bf_ref[...]
    ws_all[core] = ws_ref[...]
    tab1[landing(me), :] = gath1[slot(me), :]

    chunk = 256
    first_view = core == 0

    def view_row(ref, k):
        at = pl.ds(pl.multiple_of(k * per_tile, per_tile), per_tile)
        return jnp.where(first_view, ref[0:1, at], ref[1:2, at])

    def count_tile(k, carry):
        src = view_row(src_ref, k)
        dst = jnp.where(view_row(keep_ref, k) == 1, view_row(dst_ref, k) - k * TILE, -1)
        row_at = lax.broadcasted_iota(jnp.int32, (TILE, per_tile), 0)
        hits = jnp.where(row_at == dst, 1.0, 0.0)
        at = pl.ds(pl.multiple_of(k * TILE, TILE), TILE)
        deg[at, :] = 1.0 / (1.0 + jnp.sum(hits, axis=1, keepdims=True))
        hits = hits.astype(BF16)

        def count_chunk(c, inner):
            source_at = lax.broadcasted_iota(jnp.int32, (chunk, per_tile), 0)
            hot = jnp.where(source_at == src - c * chunk, 1.0, 0.0).astype(BF16)
            counts = lax.dot_general(hits, hot, (((1,), (1,)), ((), ())), preferred_element_type=F32)
            self_row = lax.broadcasted_iota(jnp.int32, (TILE, chunk), 0) + k * TILE
            self_col = lax.broadcasted_iota(jnp.int32, (TILE, chunk), 1) + c * chunk
            counts = counts + jnp.where(self_row == self_col, 1.0, 0.0)
            high = counts.astype(BF16)
            cols = pl.ds(pl.multiple_of(c * chunk, chunk), chunk)
            a_hi[at, cols] = high
            a_lo[at, cols] = (counts - high.astype(F32)).astype(BF16)
            return inner

        lax.fori_loop(0, sources // chunk, count_chunk, 0)
        return carry

    lax.fori_loop(0, tiles, count_tile, 0)

    depth = 512 if sources % 512 == 0 else 256

    def mixed(table, c):
        cols = pl.ds(pl.multiple_of(c * depth, depth), depth)
        part = table[cols, :]
        return dot(a_hi[:, cols], part) + dot(a_lo[:, cols], part)

    drain(tab1.at[pl.ds(rows, others * halo)], recv_sem.at[0])
    summed = lax.fori_loop(
        0, sources // depth, lambda c, total: total + mixed(tab1, c), jnp.zeros((rows, width), F32))
    mean = summed * deg[...]
    tabm[0:rows, :] = mean
    parts3 = split(mean, 3)

    def gather_mean(c, carry):
        at = pl.ds(pl.multiple_of(c * step_rows, step_rows), step_rows)
        hot = pick[at, :]
        gath2[at, :] = dot(hot, parts3[0]) + (dot(hot, parts3[1]) + dot(hot, parts3[2]))
        return carry

    lax.fori_loop(0, out_rows // step_rows, gather_mean, 0)
    each(lambda to: remote(
        gath2.at[slot(to)], tabm.at[landing(me)], send_sem.at[1], recv_sem.at[1], to, core).start())
    tabm[landing(me), :] = gath2[slot(me), :]
    for copy in weights:
        copy.wait_recv()

    def rows_of(c):
        at = pl.ds(pl.multiple_of(c * depth, depth), depth)
        wide = jnp.concatenate(split(tabm[at, :], 2), axis=1)
        for h in range(feats):
            w = wf_all[h]
            proj = dot(wide, jnp.concatenate([w, w], axis=0))
            hid[:, h * half:(h + 1) * half] = jnp.maximum(proj + bf_all[h], 0.0).astype(BF16)
        for h in range(feats):
            tab2[at, h * half:(h + 1) * half] = dot(hid[...], ws_all[h]).astype(BF16)

    local = rows // depth
    for c in range(local):
        rows_of(c)
        if c == 0:
            acc[...] = mixed(tab2, c)
        else:
            acc[...] += mixed(tab2, c)
    drain(tabm.at[pl.ds(rows, others * halo)], recv_sem.at[1])

    def add_chunk(c, carry):
        rows_of(c)
        acc[...] += mixed(tab2, c)
        return carry

    lax.fori_loop(local, sources // depth, add_chunk, 0)

    live_count = count_ref[0]
    live = lax.broadcasted_iota(jnp.int32, (rows, 1), 0) < live_count
    mine_count = live_count.astype(F32)
    blocks = emb // TILE
    for q in range(blocks):
        cols = slice(q * TILE, (q + 1) * TILE)
        value = acc[:, cols] * deg[...]
        acc[:, cols] = value
        total = jnp.sum(jnp.where(live, value, 0.0), axis=0, keepdims=True)
        off = jnp.where(live, value - total / mine_count, 0.0)
        st_own[q:q + 1, :] = total
        st_own[blocks + q:blocks + q + 1, :] = jnp.sum(off * off, axis=0, keepdims=True)
    tail = st_own.shape[0] - 2 * blocks
    st_own[2 * blocks:, :] = jnp.zeros((tail, TILE), F32) + mine_count
    each(lambda to: remote(
        st_own, st_all.at[me], send_sem.at[2], recv_sem.at[2], to, core).start())
    st_all[me] = st_own[...]
    drain(st_all.at[pl.ds(0, others)], recv_sem.at[2])
    sizes = st_all[:, 2 * blocks:2 * blocks + 1, :]
    sums = st_all[:, 0:blocks, :]
    spreads = st_all[:, blocks:2 * blocks, :]
    node_total = jnp.sum(sizes, axis=0)
    average = jnp.sum(sums, axis=0) / node_total
    shift = sums / sizes - average[None]
    variance = jnp.sum(spreads + sizes * shift * shift, axis=0) / node_total
    scale = 1.0 / jnp.sqrt(variance + 1e-05)
    for q in range(blocks):
        value = (acc[:, q * TILE:(q + 1) * TILE] - average[q:q + 1, :]) * scale[q:q + 1, :]
        per_half = half // TILE
        at = (q % per_half) * TILE
        mine[q // per_half, :, at:at + TILE] = jnp.where(live, value, 0.0).astype(BF16)

    swap = remote(mine.at[mate], other.at[mate], n_send.at[0], n_recv.at[0], me, mate)
    extra = remote(mine.at[core], other.at[core], n_send.at[1], n_recv.at[1], me, mate)
    swap.start()

    @pl.when(first_view)
    def _():
        extra.start()

    normed_ref[core] = mine[core]
    contract = (((0,), (0,)), ((), ()))

    def put(h, product):
        per = half // share
        for j in range(per):
            p_send[h * per + j] = product[j * share:(j + 1) * share, :]

    swap.wait_recv()
    normed_ref[mate] = other[core]

    @pl.when(first_view)
    def _():
        for h in range(feats):
            put(h, lax.dot_general(mine[h], other[0], contract, preferred_element_type=F32))

    @pl.when(jnp.logical_not(first_view))
    def _():
        put(1, lax.dot_general(other[1], mine[1], contract, preferred_element_type=F32))
        pltpu.make_async_copy(other.at[0], other.at[0], n_recv.at[1]).wait()
        put(0, lax.dot_general(other[0], mine[1], contract, preferred_element_type=F32))

    each(lambda to: remote(
        p_send.at[to], p_recv.at[me], send_sem.at[3], recv_sem.at[3], to, core).start())
    p_recv[me] = p_send[me]
    drain(p_recv.at[pl.ds(0, others)], recv_sem.at[3])
    total = node_total[:, 0:1]
    corr = jnp.sum(p_recv[...], axis=0) / total
    corr_ref[...] = corr
    row_label = lax.broadcasted_iota(jnp.int32, (share, half), 0) + me * share
    col_label = lax.broadcasted_iota(jnp.int32, (share, half), 1) + core * half
    miss = 1.0 - corr
    terms = jnp.where(row_label == col_label, miss * miss, 0.005 * (corr * corr))
    line = jnp.sum(terms, axis=0, keepdims=True)
    folded = line[:, 0:TILE]
    for q in range(1, half // TILE):
        folded = folded + line[:, q * TILE:(q + 1) * TILE]
    l_own[...] = folded
    pair = remote(l_own, l_mate, n_send.at[2], n_recv.at[2], me, mate)
    pair.start()
    pair.wait_recv()
    both = folded + l_mate[...]
    l_sum[...] = both
    each(lambda to: remote(
        l_sum, l_all.at[me], send_sem.at[4], recv_sem.at[4], to, core).start())
    l_all[me] = both
    drain(l_all.at[pl.ds(0, others)], recv_sem.at[4])
    loss_ref[0, 0] = jnp.sum(l_all[...])

    for copy in weights:
        copy.wait_send()
    swap.wait_send()

    @pl.when(first_view)
    def _():
        extra.wait_send()

    drain(gath1.at[pl.ds(0, others * halo)], send_sem.at[0])
    drain(gath2.at[pl.ds(0, others * halo)], send_sem.at[1])
    drain(st_all.at[pl.ds(0, others)], send_sem.at[2])
    drain(p_send.at[pl.ds(0, others)], send_sem.at[3])
    pair.wait_send()
    drain(l_all.at[pl.ds(0, others)], send_sem.at[4])


def per_device(
    features, row_counts, send_rows, edge_src, edge_dst, edge_keep, w_first, b_first, w_second
):
    parts = lax.axis_size("nodes")
    feats = lax.axis_size("feat")
    rows, width = features.shape
    halo = send_rows.shape[2]
    half = w_first.shape[1]
    hidden, emb_half = w_second.shape
    emb = emb_half * feats
    share = emb // parts
    sources = rows + parts * halo
    blocks = emb // TILE
    vmem = pl.BlockSpec(memory_space=pltpu.VMEM)
    smem = pl.BlockSpec(memory_space=pltpu.SMEM)
    pad_rows = -(-parts // TILE) * TILE
    normed, correlation, loss = pl.pallas_call(
        functools.partial(kernel, parts, feats),
        out_shape=(
            jax.ShapeDtypeStruct((2, rows, emb_half), BF16),
            jax.ShapeDtypeStruct((share, emb_half), F32),
            jax.ShapeDtypeStruct((1, 1), F32),
        ),
        in_specs=[vmem, smem] + [vmem] * 7,
        out_specs=(vmem, vmem, smem),
        scratch_shapes=[
            pltpu.VMEM((pad_rows, TILE), F32),
            pltpu.VMEM((parts * halo, rows), BF16),
            pltpu.VMEM((parts * halo, width), BF16),
            pltpu.VMEM((sources, width), BF16),
            pltpu.VMEM((parts * halo, width), F32),
            pltpu.VMEM((sources, width), F32),
            pltpu.VMEM((sources, emb), BF16),
            pltpu.VMEM((rows, sources), BF16),
            pltpu.VMEM((rows, sources), BF16),
            pltpu.VMEM((rows, 1), F32),
            pltpu.VMEM((feats, width, half), BF16),
            pltpu.VMEM((feats, 1, half), F32),
            pltpu.VMEM((feats, hidden, emb_half), BF16),
            pltpu.VMEM((512 if sources % 512 == 0 else 256, hidden), BF16),
            pltpu.VMEM((rows, emb), F32),
            pltpu.VMEM((2 * blocks + 8, TILE), F32),
            pltpu.VMEM((parts, 2 * blocks + 8, TILE), F32),
            pltpu.VMEM((feats, rows, emb_half), BF16),
            pltpu.VMEM((feats, rows, emb_half), BF16),
            pltpu.VMEM((parts, share, emb_half), F32),
            pltpu.VMEM((parts, share, emb_half), F32),
            pltpu.VMEM((1, TILE), F32),
            pltpu.VMEM((1, TILE), F32),
            pltpu.VMEM((1, TILE), F32),
            pltpu.VMEM((parts, 1, TILE), F32),
            pltpu.SemaphoreType.DMA((5,)),
            pltpu.SemaphoreType.DMA((5,)),
            pltpu.SemaphoreType.DMA((3,)),
            pltpu.SemaphoreType.DMA((3,)),
            pltpu.SemaphoreType.DMA((3,)),
            pltpu.SemaphoreType.DMA((3,)),
        ],
        compiler_params=pltpu.CompilerParams(
            collective_id=0, has_side_effects=True, vmem_limit_bytes=60 * 1024 * 1024
        ),
    )(
        features, row_counts, send_rows, edge_src, edge_dst, edge_keep, w_first,
        b_first.reshape(1, half), w_second,
    )
    return normed, correlation, loss.reshape(())


def solution(mesh):
    placed = (
        P("nodes", None),
        P("nodes"),
        P("nodes", None, None),
        P(None, "nodes"),
        P(None, "nodes"),
        P(None, "nodes"),
        P(None, "feat"),
        P("feat"),
        P(None, "feat"),
    )
    return jax.shard_map(
        per_device,
        mesh=mesh,
        in_specs=placed,
        out_specs=(P(None, "nodes", "feat"), P("nodes", "feat"), P()),
        check_vma=False,
    )
```
